32 devices in a mesh: ctx: 4 (over x, core), vocab: 8 (over z, y).
Axes of the slice: x: 2, y: 2, z: 4, core: 2. Of those that a mesh axis runs over, the one named last changes fastest.
Arguments:
- hidden: bfloat16 [256, 2, 7168], P('ctx', None, 'vocab'), may hold values from -30 to 30
- head: bfloat16 [7168, 16384], P('ctx', 'vocab'), may hold values from -0.15 to 0.15
- targets: int32 [256, 2], P('ctx'), may hold values from 0 to 16383
- loss_weight: float32 [256, 2], P('ctx'), may hold values from 16 to 256
Outputs:
- token_loss: float32 [256, 2], P('ctx')
- grad_hidden: bfloat16 [256, 2, 7168], P('ctx', None, 'vocab')
The draws below stay inside these ranges and needn't reach their ends.
All inputs are finite; a program needn't handle non-finite values.
Results may differ from the reference program's by a relative error of at most 0.0046.
Values may be sent and summed in bfloat16 or wider, within the bound.
No kernel may reach another device: no remote copies, remote signals or barrier semaphores. Data moves between devices by JAX's collectives and lax.ppermute only.
A program may use at most 64 MiB of HBM per device.

```python
import math
import jax
import jax.numpy as jnp
import numpy as np
from jax import lax

D = 7168
DEPTHS = 2
TOKENS = 256
VOCAB = 16384


def draw_hidden(key, part):
    draw_base = jnp.clip(jax.random.normal(jax.random.fold_in(key, 1), (TOKENS, DEPTHS, D), jnp.float32), -6.0, 6.0)
    return draw_base.astype(jnp.bfloat16)


def draw_head(key, part):
    scale_col = D ** (-0.5)
    draw_base = jnp.clip(jax.random.normal(jax.random.fold_in(key, 4), (D, VOCAB), jnp.float32), -6.0, 6.0) * scale_col
    draw_base = jnp.clip(draw_base, -0.149, 0.149)
    return draw_base.astype(jnp.bfloat16)


def touch_ends(values, own_key, least, high):
    index_at = [jax.random.randint(jax.random.fold_in(own_key, axis), (), 0, length) for axis, length in enumerate(values.shape)]
    main_axis = values.shape.index(max(values.shape))
    next_to = index_at[:main_axis] + [(index_at[main_axis] + 1) % values.shape[main_axis]] + index_at[main_axis + 1:]
    return values.at[tuple(index_at)].set(least).at[tuple(next_to)].set(high)


def levels(rng, dims, pieces, low, largest):
    level, own = 1.0, jax.random.fold_in(rng, 6)
    for axis_at, blocks in pieces:
        heights = jnp.exp(jax.random.uniform(jax.random.fold_in(own, axis_at), (blocks,), jnp.float32, low / len(pieces), largest / len(pieces)))
        level = level * jnp.repeat(heights, dims[axis_at] // blocks).reshape([-1 if axis == axis_at else 1 for axis in range(len(dims))])
    return level


def rank_table(count, slope):
    loads = [(1 << 20) // math.isqrt(standing ** slope) + 1 for standing in range(1, count + 1)]
    scale = 1 + sum(loads) // (1 << 30)
    return np.cumsum(np.array([max(1, weight // scale) for weight in loads]))


def skewed_ids(stream_key, dims, number_of, slope):
    grid = rank_table(number_of, slope)
    lot = jax.random.randint(jax.random.fold_in(stream_key, 1), dims, 0, int(grid[number_of - 1]))
    grade = jnp.searchsorted(jnp.asarray(grid, jnp.int32), lot, side="right")
    return jax.random.permutation(jax.random.fold_in(stream_key, 2), number_of)[grade].astype(jnp.int32)


def setup_inputs(seed: int = 0) -> dict:
    key_of = jax.random.split(jax.random.key(seed), 5)
    hidden = draw_hidden(jax.random.fold_in(key_of[4], 71), 0)
    head = draw_head(jax.random.fold_in(key_of[4], 71), 0)
    targets = touch_ends(skewed_ids(key_of[2], (TOKENS, DEPTHS), VOCAB, 2), jax.random.fold_in(key_of[2], 3), 0, VOCAB - 1).astype(jnp.int32)
    loss_weight = jnp.clip(jnp.exp(math.log(256.0) - 2.7725887 * jax.random.uniform(key_of[3], (TOKENS, DEPTHS), jnp.float32) ** levels(key_of[3], (TOKENS, DEPTHS), ((0, 4),), -0.2, 0.2)), 16.0, 256.0)
    return {"hidden": hidden, "head": head, "targets": targets, "loss_weight": loss_weight}


def reference(hidden, head, targets, loss_weight):
    flat_rows = hidden.reshape(TOKENS * DEPTHS, D)
    labels = targets.reshape(TOKENS * DEPTHS)
    weights = loss_weight.reshape(TOKENS * DEPTHS)
    logits = jnp.dot(flat_rows, head, preferred_element_type=jnp.float32)
    row_max = jnp.max(logits, axis=1)
    exps = jnp.exp(logits - row_max[:, None])
    sum_exp = jnp.sum(exps, axis=1)
    target_logit = jnp.take_along_axis(logits, labels[:, None], axis=1)[:, 0]
    token_loss = jnp.log(sum_exp) + row_max - target_logit
    columns = lax.broadcasted_iota(jnp.int32, logits.shape, 1)
    onehot = (columns == labels[:, None]).astype(jnp.float32)
    dlogits = (weights[:, None] * (exps / sum_exp[:, None] - onehot)).astype(jnp.bfloat16)
    grad_rows = jnp.dot(dlogits, head.T, preferred_element_type=jnp.float32).astype(jnp.bfloat16)
    return token_loss.reshape(TOKENS, DEPTHS), grad_rows.reshape(TOKENS, DEPTHS, D)
```

```python
import jax
import jax.numpy as jnp
from jax import lax
from jax.sharding import PartitionSpec as P

AXES = ("ctx", "vocab")


def make_body(ctx_count, vocab_count):
    cores = 2
    cx_count = ctx_count // cores
    slices = vocab_count // ctx_count
    rh_count = slices // 2
    high_count = vocab_count // 2

    def permute(array, target):
        pairs = []
        for source in range(ctx_count * vocab_count):
            c, v = divmod(source, vocab_count)
            c2, v2 = target(c, v)
            pairs.append((source, c2 * vocab_count + v2))
        return lax.ppermute(array, AXES, pairs)

    def flip_low(array):
        return permute(array, lambda c, v: (c, v ^ 1))

    def flip_core(array):
        return permute(array, lambda c, v: (c ^ 1, v))

    def flip_cx(array, d):
        return permute(array, lambda c, v: (c ^ (2 * d), v))

    def place(c, rh):
        return ((c % cores) * cx_count + c // cores) * rh_count + rh

    def spread(array, j):
        def target(c, v):
            slice_c, rh = divmod(v >> 1, rh_count)
            return slice_c, ((place(c, rh) ^ j) << 1) | (v & 1)

        return permute(array, target)

    def collect(array, jx, jk, jr):
        def target(c, v):
            cx, k = divmod(c, cores)
            vx, rest = divmod(v >> 1, cores * rh_count)
            vk, vr = divmod(rest, rh_count)
            high = ((vx ^ jx) * cores + k) * rh_count + (vr ^ jr)
            return cx * cores + (vk ^ jk), (high << 1) | (v & 1)

        return permute(array, target)

    def body(hidden, head, targets, loss_weight):
        group_rows, depth_count, width = hidden.shape
        rows = group_rows * depth_count
        vocab_local = head.shape[1]
        total = ctx_count * rows
        c = lax.axis_index("ctx")
        v = lax.axis_index("vocab")
        cx, k = c // cores, c % cores
        vh, y = v // 2, v % 2
        flat_hidden = hidden.reshape(rows, width)
        flat_targets = targets.reshape(rows)
        flat_weights = loss_weight.reshape(rows)

        own = jnp.zeros((rh_count, ctx_count, rows, width), jnp.bfloat16)
        other = own
        for j in range(high_count):
            block = spread(flat_hidden, j)
            mate = flip_low(block)
            at = vh ^ j
            owner, rh = at // rh_count, at % rh_count
            index = (rh, (owner % cx_count) * cores + owner // cx_count, 0, 0)
            own = lax.dynamic_update_slice(own, block[None, None], index)
            other = lax.dynamic_update_slice(other, mate[None, None], index)
        own = own.reshape(rh_count, total, width)
        other = other.reshape(rh_count, total, width)
        parts = []
        for rh in range(rh_count):
            parts.append(jnp.where(y == 0, own[rh], other[rh]))
            parts.append(jnp.where(y == 0, other[rh], own[rh]))
        features = jnp.concatenate(parts, axis=1)

        partial = jnp.dot(features, head, preferred_element_type=jnp.float32)
        partial = partial.reshape(cx_count, cores, rows, vocab_local)
        away = jnp.where(k == 0, partial[:, 1], partial[:, 0])
        home = jnp.where(k == 0, partial[:, 0], partial[:, 1])
        chip_sum = home + flip_core(away)
        logits = lax.dynamic_index_in_dim(chip_sum, cx, 0, keepdims=False)
        for d in range(1, cx_count):
            logits += flip_cx(lax.dynamic_index_in_dim(chip_sum, cx ^ d, 0, keepdims=False), d)

        columns = v * vocab_local + lax.broadcasted_iota(jnp.int32, logits.shape, 1)
        target_hit = columns == flat_targets[:, None]
        row_max = jnp.max(logits, axis=1)
        sum_exp = jnp.sum(jnp.exp(logits - row_max[:, None]), axis=1)
        target_logit = jnp.sum(jnp.where(target_hit, logits, 0.0), axis=1)
        step = 1
        while step < vocab_count:
            got = permute(jnp.stack([row_max, sum_exp, target_logit]), lambda c, v, s=step: (c, v ^ s))
            new_max = jnp.maximum(row_max, got[0])
            sum_exp = sum_exp * jnp.exp(row_max - new_max) + got[1] * jnp.exp(got[0] - new_max)
            target_logit = target_logit + got[2]
            row_max = new_max
            step *= 2
        token_loss = (jnp.log(sum_exp) + row_max - target_logit).reshape(group_rows, depth_count)
        probabilities = jnp.exp(logits - row_max[:, None]) / sum_exp[:, None]
        dlogits = (flat_weights[:, None] * (probabilities - target_hit.astype(jnp.float32))).astype(jnp.bfloat16)

        gathered = jnp.zeros((cx_count, rows, vocab_local), jnp.bfloat16)
        gathered = lax.dynamic_update_slice(gathered, dlogits[None], (cx, 0, 0))
        for d in range(1, cx_count):
            gathered = lax.dynamic_update_slice(gathered, flip_cx(dlogits, d)[None], (cx ^ d, 0, 0))
        mate = flip_core(gathered)
        low = jnp.where(k == 0, gathered, mate)
        high = jnp.where(k == 0, mate, gathered)
        all_dlogits = jnp.stack([low, high], axis=1).reshape(total, vocab_local)

        grad = lax.dot_general(
            all_dlogits, head, (((1,), (1,)), ((), ())), preferred_element_type=jnp.float32
        )
        keep, send = [], []
        for rh in range(rh_count):
            first = grad[:, 2 * rh * width : (2 * rh + 1) * width]
            second = grad[:, (2 * rh + 1) * width : (2 * rh + 2) * width]
            keep.append(jnp.where(y == 0, first, second))
            send.append(jnp.where(y == 0, second, first).astype(jnp.bfloat16))
        summed = jnp.stack(keep) + flip_low(jnp.stack(send)).astype(jnp.float32)
        summed = summed.astype(jnp.bfloat16).reshape(rh_count, cx_count, cores * rows, width)
        held = jnp.zeros((cx_count, rh_count, cores * rows, width), jnp.bfloat16)
        mine = lax.dynamic_index_in_dim(summed, cx, 1, keepdims=False)
        held = lax.dynamic_update_slice(held, mine[None], (cx, 0, 0, 0))
        for d in range(1, cx_count):
            moved = flip_cx(lax.dynamic_index_in_dim(summed, cx ^ d, 1, keepdims=False), d)
            held = lax.dynamic_update_slice(held, moved[None], (cx ^ d, 0, 0, 0))
        held = held.reshape(cx_count, rh_count, cores, rows, width)
        vx, rest = vh // (cores * rh_count), vh % (cores * rh_count)
        vk, vr = rest // rh_count, rest % rh_count
        grad_out = None
        for jx in reversed(range(cx_count)):
            for jk in range(cores):
                for jr in range(rh_count):
                    block = lax.dynamic_slice(
                        held, (vx ^ jx, vr ^ jr, vk ^ jk, 0, 0), (1, 1, 1, rows, width)
                    ).reshape(rows, width)
                    got = collect(block, jx, jk, jr).astype(jnp.float32)
                    grad_out = got if grad_out is None else grad_out + got
        grad_out = grad_out.astype(jnp.bfloat16).reshape(group_rows, depth_count, width)
        return (token_loss, grad_out)

    return body


def solution(mesh):
    return jax.shard_map(
        make_body(mesh.shape["ctx"], mesh.shape["vocab"]),
        mesh=mesh,
        in_specs=(P("ctx", None, "vocab"), P("ctx", "vocab"), P("ctx", None), P("ctx", None)),
        out_specs=(P("ctx", None), P("ctx", None, "vocab")),
        check_vma=False,
    )
```
